128 devices in a mesh: section: 2 (over z_hi), row: 8 (over x, core), col: 8 (over y, z_lo).
Axes of the slice: x: 4, y: 4, z: 4 (z_hi: 2, z_lo: 2; z = z_hi * 2 + z_lo), core: 2. Of those that a mesh axis runs over, the one named last changes fastest.
Arguments:
- inputs: float32 [3, 128, 16384], P(None, None, ('row', 'col')), may hold values from -512 to 512
- weights: float32 [2, 8, 8, 256, 16384], P('section', None, 'col', None, 'row'), may hold values from -1 to 1
- norm_gain: float32 [2, 16384], P('section', ('row', 'col')), may hold values from 0.5 to 1.5
Outputs:
- section_outputs: float32 [2, 3, 128, 16384], P('section', None, None, ('row', 'col'))
The draws below stay inside these ranges and needn't reach their ends.
All inputs are finite; a program needn't handle non-finite values.
Results may differ from the reference program's by a relative error of at most 0.00036.
Values sent between devices are 32-bit elements; how exact they have to be, the bound alone decides.
A program may use at most 128 MiB of HBM per device.

```python
import math
import jax
import jax.numpy as jnp
from jax import lax

D = 16384
B = 128
M = 3
LAYERS = 2
ROW_BLOCKS = 8
COL_BLOCKS = 8
PIECE = 256


offset_scale = 64.0


def shared_basis(key):
    raw_draw = jax.random.normal(jax.random.fold_in(key, 7103), (D, M * B), jnp.float32)
    basis_cols, upper_part = jnp.linalg.qr(raw_draw)
    return basis_cols


def draw_inputs(key, part):
    basis_cols = shared_basis(key)
    count = M * B
    mixing = jax.random.normal(jax.random.fold_in(key, 211), (count, count), jnp.float32) / math.sqrt(count)
    amplitude = jnp.ones((count, 1), jnp.float32)
    rough = jax.random.normal(jax.random.fold_in(key, 229), (count, D), jnp.float32)
    along = jnp.dot(mixing, basis_cols.T, precision=lax.Precision.HIGHEST)
    large = offset_scale * math.sqrt(D) * amplitude * along
    values = jnp.clip(large + rough, -512.0, 512.0)
    return values.reshape(M, B, D)


def draw_weights(key, part):
    basis_cols = shared_basis(key)
    matrices = []
    for level in range(LAYERS):
        layer_key = jax.random.fold_in(key, 401 + level)
        dense = jnp.clip(jax.random.normal(layer_key, (D, D), jnp.float32), -6.0, 6.0) / math.sqrt(D)
        inside = jnp.dot(basis_cols.T, dense, precision=lax.Precision.HIGHEST)
        matrix = dense - (1.0 - 1.0 / offset_scale) * jnp.dot(basis_cols, inside, precision=lax.Precision.HIGHEST)
        matrices.append(matrix.reshape(ROW_BLOCKS, COL_BLOCKS, PIECE, D))
    return jnp.stack(matrices)


def setup_inputs(seed: int = 0) -> dict:
    key_of = jax.random.split(jax.random.key(seed), 4)
    return {
        "inputs": draw_inputs(jax.random.fold_in(key_of[3], 71), 0),
        "weights": draw_weights(jax.random.fold_in(key_of[3], 71), 0),
        "norm_gain": jnp.clip(1.0 + 0.1 * jax.random.normal(key_of[2], (LAYERS, D), jnp.float32), 0.5, 1.5),
    }


def split_two(values):
    first = lax.optimization_barrier(values.astype(jnp.bfloat16))
    second = lax.optimization_barrier((values - first.astype(jnp.float32)).astype(jnp.bfloat16))
    return (first, second)

def widen(values):
    return values.astype(jnp.float32)

def layer(activations, matrix, gain):
    first, second = split_two(activations)
    sum_two = widen(first) + widen(second)
    sum_one = widen(first)
    width = matrix.shape[1]
    block_cols = width // 8

    def column_block(index):
        cols = lax.dynamic_slice_in_dim(matrix, (index * block_cols).astype(jnp.int32), block_cols, 1)
        wfirst, wsecond = split_two(cols)
        total = jnp.dot(sum_two.astype(jnp.float32), widen(wfirst).astype(jnp.float32), precision=lax.Precision.HIGHEST, preferred_element_type=jnp.float32)
        total = total + jnp.dot(sum_one.astype(jnp.float32), widen(wsecond).astype(jnp.float32), precision=lax.Precision.HIGHEST, preferred_element_type=jnp.float32)
        return total
    blocks = lax.map(column_block, jnp.arange(8, dtype=jnp.int32))
    summed = jnp.transpose(blocks, (1, 0, 2)).reshape(activations.shape[0], width)
    active = jax.nn.gelu(summed, approximate=True)
    squares = lax.optimization_barrier(jnp.sum(active * active, axis=1))
    scale = lax.rsqrt(squares / width + 1e-06)
    return active * scale[:, None] * gain[None, :]

def reference(inputs, weights, norm_gain):
    current = inputs.reshape(M * B, D)
    results = []
    for level in range(LAYERS):
        matrix = weights[level].reshape(D, D)
        branch = layer(current, matrix, norm_gain[level])
        results.append(branch.reshape(M, B, D))
        current = current + branch
    return jnp.stack(results)
```

```python
import functools

import jax
import jax.numpy as jnp
from jax import lax
from jax.experimental import pallas as pl
from jax.experimental.pallas import tpu as pltpu
from jax.sharding import PartitionSpec as P

MESH = pl.DeviceIdType.MESH
F32 = jnp.float32
BF16 = jnp.bfloat16
CHUNK_ROWS = 96


def kernel(
    count, x_ref, w_ref, gain_ref, out_ref,
    wf, w1, w2, xd, g1, g2, p1s, p1r, p2s, p2r, own, zs, zr, yg, sa, sb, st, sr,
    wsem, xsem, ag_s, ag_r, p1_ss, p1_rs, p2_ss, p2_rs, z_ss, z_rs, t_ss, t_rs, st_ss, st_rs,
    sa_ss, sa_rs, sb_ss, sb_rs,
):
    sec = lax.axis_index("section")
    r = lax.axis_index("row")
    q = lax.axis_index("col")
    rows = out_ref.shape[0] // count
    half = rows // 2
    piece = out_ref.shape[1]
    features = piece * 64
    y = q // 2
    z = q % 2
    xp, xm, x2 = (r + 2) % 8, (r + 6) % 8, (r + 4) % 8
    mate = r + 1 - 2 * (r % 2)
    mp, mm_, m2 = (mate + 2) % 8, (mate + 6) % 8, (mate + 4) % 8
    yp, ym = (q + 2) % 8, (q + 6) % 8
    zmate = q + 1 - 2 * z
    to_xp, to_xm, to_mate = {"row": xp}, {"row": xm}, {"row": mate}
    to_yp, to_ym, to_z = {"col": yp}, {"col": ym}, {"col": zmate}
    to_next = {"section": 1 - sec}

    def cp(src, dst, ss, rs, dev):
        return pltpu.make_async_remote_copy(
            src_ref=src, dst_ref=dst, send_sem=ss, recv_sem=rs, device_id=dev, device_id_type=MESH
        )

    def block(off):
        return (y + off) % 4

    offs = (2, 1, 3, 0)

    def wcopy(k):
        nb = block(offs[k // 2]) * 2 + k % 2
        cols = pl.ds(pl.multiple_of(nb * piece, piece), piece)
        return pltpu.make_async_copy(w_ref.at[:, cols], wf.at[nb], wsem.at[k]), nb

    xcopy = pltpu.make_async_copy(x_ref, g1.at[r], xsem)
    xcopy.start()
    for k in range(8):
        wcopy(k)[0].start()

    peers = [{"row": (r + d) % 8} for d in range(1, 8)]
    peers += [{"col": (q + d) % 8} for d in range(1, 8)]
    peers += [to_next]
    barrier = pltpu.get_barrier_semaphore()
    for dev in peers:
        pl.semaphore_signal(barrier, inc=1, device_id=dev, device_id_type=MESH)
    pl.semaphore_wait(barrier, len(peers))
    xcopy.wait()

    def rs(c):
        return pl.ds(c * rows, rows)

    def ra(c):
        return pl.ds(c * rows, half)

    def rb(c):
        return pl.ds(c * rows + half, half)

    def ag(g, n, c, j):
        src = (
            (r, rs(c)), (r, rs(c)), (r, rs(c)), (xm, ra(c)), (xp, rb(c)),
            (xm, rs(c)), (xp, rs(c)), (x2, ra(c)), (x2, rb(c)),
        )[j]
        dev = (to_xp, to_xm, to_mate, to_xp, to_xm, to_mate, to_mate, to_mate, to_mate)[j]
        ref = g.at[src[0], src[1], :]
        return cp(ref, ref, ag_s.at[n, c, j], ag_r.at[n, c, j], dev)

    def ag_in(g, n, c, j):
        dst = (
            (xm, rs(c)), (xp, rs(c)), (mate, rs(c)), (x2, ra(c)), (x2, rb(c)),
            (mm_, rs(c)), (mp, rs(c)), (m2, ra(c)), (m2, rb(c)),
        )[j]
        ref = g.at[dst[0], dst[1], :]
        return cp(ref, ref, ag_s.at[n, c, j], ag_r.at[n, c, j], to_mate)

    def ag1(g, n, c):
        for j in (0, 1, 2):
            ag(g, n, c, j).start()

    def ag2(g, n, c):
        ag_in(g, n, c, 0).wait_recv()
        ag(g, n, c, 3).start()
        ag(g, n, c, 5).start()
        ag_in(g, n, c, 1).wait_recv()
        ag(g, n, c, 4).start()
        ag(g, n, c, 6).start()

    def ag3(g, n, c):
        ag_in(g, n, c, 3).wait_recv()
        ag(g, n, c, 7).start()
        ag_in(g, n, c, 4).wait_recv()
        ag(g, n, c, 8).start()

    def ag4(g, n, c):
        for j in (2, 5, 6, 7, 8):
            ag_in(g, n, c, j).wait_recv()

    def ag_done(g, n, c):
        for j in range(9):
            ag(g, n, c, j).wait_send()

    def slice_weights(ks):
        for k in ks:
            copy, nb = wcopy(k)
            copy.wait()

            def body(t, carry, nb=nb):
                rr = pl.ds(pl.multiple_of(t * 256, 256), 256)
                v = wf[nb, rr, :]
                a = v.astype(BF16)
                w1[nb, rr, :] = a
                w2[nb, rr, :] = (v - a.astype(F32)).astype(BF16)
                return carry

            lax.fori_loop(0, 8, body, 0)

    def as_row(v):
        h = v[:, :128] + v[:, 128:]
        if rows < 128:
            h = jnp.concatenate([h, jnp.zeros((128 - rows, 128), F32)], axis=0)
        t = jnp.sum(jnp.transpose(h), axis=0, keepdims=True)
        return jnp.broadcast_to(t, (8, 128))

    def scale_of(total):
        inv = lax.rsqrt(total / features + 1e-06)
        t = jnp.transpose(jnp.broadcast_to(inv[:1], (128, 128)))[:rows]
        return jnp.concatenate([t, t], axis=1)

    def split_into(i, v):
        a = v.astype(BF16)
        cols = pl.ds(i * piece, piece)
        xd[0:rows, cols] = a
        xd[rows : 2 * rows, cols] = (v - a.astype(F32)).astype(BF16)

    def mm(off, dst):
        base = block(off) * 2

        def body(zz, carry):
            a = jnp.dot(xd[...], w1[base + zz], preferred_element_type=F32)
            b = jnp.dot(xd[0:rows, :], w2[base + zz], preferred_element_type=F32)
            dst[zz] = a[:rows] + a[rows:] + b
            return carry

        lax.fori_loop(0, 2, body, 0)

    A, B = pl.ds(0, half), pl.ds(half, half)

    def p1(c, j):
        part, dev = ((A, to_yp), (B, to_ym))[j]
        return cp(p1s.at[c, :, part, :], p1r.at[c, :, part, :], p1_ss.at[c, j], p1_rs.at[c, j], dev)

    def p2(c, j):
        d, part, dev = ((0, B, to_yp), (1, A, to_ym), (0, A, to_yp), (1, B, to_ym))[j]
        return cp(
            p2s.at[c, d, :, part, :], p2r.at[c, d, :, part, :], p2_ss.at[c, j], p2_rs.at[c, j], dev
        )

    def f1(c):
        p1(c, 0).wait_recv()
        p2s[c, 0, :, 0:half, :] = p2s[c, 0, :, 0:half, :] + p1r[c, :, 0:half, :]
        p2(c, 2).start()
        p1(c, 1).wait_recv()
        p2s[c, 1, :, half:rows, :] = p2s[c, 1, :, half:rows, :] + p1r[c, :, half:rows, :]
        p2(c, 3).start()

    def zcopy(c):
        return cp(zs.at[c], zr.at[c], z_ss.at[c], z_rs.at[c], to_z)

    def f2(c):
        for j in range(4):
            p2(c, j).wait_recv()
        zs[c] = own[c, 1 - z] + p2r[c, 0, 1 - z] + p2r[c, 1, 1 - z]
        zcopy(c).start()
        own[c, z] = own[c, z] + p2r[c, 0, z] + p2r[c, 1, z]

    def tcopy(c):
        return cp(yg.at[rs(c), :], g2.at[r, rs(c), :], t_ss.at[c], t_rs.at[c], to_next)

    def sacopy(c, d):
        return cp(sa.at[c, r], sa.at[c, r], sa_ss.at[c], sa_rs.at[c], {"row": (r + d) % 8})

    def sbcopy(c, d):
        return cp(sb.at[c, q], sb.at[c, q], sb_ss.at[c], sb_rs.at[c], {"col": (q + d) % 8})

    def sa_all(c):
        ref = sa.at[c, pl.ds(0, 7)]
        return cp(ref, ref, sa_ss.at[c], sa_rs.at[c], to_mate)

    def sb_all(c):
        ref = sb.at[c, pl.ds(0, 7)]
        return cp(ref, ref, sb_ss.at[c], sb_rs.at[c], to_z)

    def f3(c):
        zcopy(c).wait_recv()
        v = jax.nn.gelu(own[c, z] + zr[c], approximate=True)
        yg[rs(c), :] = v * gain_ref[...]

        @pl.when(sec == 0)
        def _():
            tcopy(c).start()

        sa[c, r] = as_row(v * v)
        for d in range(1, 8):
            sacopy(c, d).start()

    def f4(c):
        sa_all(c).wait_recv()
        t = sa[c, 0]
        for i in range(1, 8):
            t = t + sa[c, i]
        sb[c, q] = t
        for d in range(1, 8):
            sbcopy(c, d).start()

    def stcopy(c):
        return cp(st.at[c], sr.at[c], st_ss.at[c], st_rs.at[c], to_next)

    def f5(c):
        sb_all(c).wait_recv()
        t = sb[c, 0]
        for i in range(1, 8):
            t = t + sb[c, i]

        @pl.when(sec == 0)
        def _():
            st[c] = t
            stcopy(c).start()

        out_ref[rs(c), :] = yg[rs(c), :] * scale_of(t)

    ag1(g1, 0, 0)
    slice_weights((0, 1, 2, 3))
    ag2(g1, 0, 0)
    ag1(g1, 0, 1)
    slice_weights((4, 5, 6, 7))
    ag3(g1, 0, 0)
    ag2(g1, 0, 1)
    if count > 2:
        ag1(g1, 0, 2)

    @pl.when(sec == 1)
    def _():
        for c in range(1, count):
            ag3(g1, 0, c)
            if c + 1 < count:
                ag2(g1, 0, c + 1)
            if c + 2 < count:
                ag1(g1, 0, c + 2)
        for c in range(count):
            ag4(g1, 0, c)

    for c in range(count):

        @pl.when(sec == 0)
        def _(c=c):
            ag4(g1, 0, c)
            for i in range(8):
                split_into(i, g1[i, rs(c), :])

        @pl.when(sec == 1)
        def _(c=c):
            tcopy(c).wait_recv()
            ag1(g2, 1, c)
            ag2(g2, 1, c)
            ag3(g2, 1, c)
            ag4(g2, 1, c)
            stcopy(c).wait_recv()
            scale = scale_of(sr[c])
            for i in range(8):
                split_into(i, g1[i, rs(c), :] + g2[i, rs(c), :] * scale)

        mm(2, p1s.at[c])
        p1(c, 0).start()
        p1(c, 1).start()
        if c:
            f2(c - 1)
        mm(1, p2s.at[c, 0])
        p2(c, 0).start()
        if c:
            f3(c - 1)
        mm(3, p2s.at[c, 1])
        p2(c, 1).start()
        f1(c)
        if c:
            f4(c - 1)
        mm(0, own.at[c])
        if c:
            f5(c - 1)

        @pl.when(sec == 0)
        def _(c=c):
            if c + 1 < count:
                ag3(g1, 0, c + 1)
            if c + 2 < count:
                ag2(g1, 0, c + 2)
            if c + 3 < count:
                ag1(g1, 0, c + 3)

    last = count - 1
    f2(last)
    f3(last)
    f4(last)
    f5(last)

    for c in range(count):
        ag_done(g1, 0, c)
        for j in range(2):
            p1(c, j).wait_send()
        for j in range(4):
            p2(c, j).wait_send()
        zcopy(c).wait_send()
        sa_all(c).wait_send()
        sb_all(c).wait_send()

    @pl.when(sec == 0)
    def _():
        for c in range(count):
            tcopy(c).wait_send()
            stcopy(c).wait_send()

    @pl.when(sec == 1)
    def _():
        for c in range(count):
            ag_done(g2, 1, c)


def shards(inputs, weights, norm_gain):
    micro, batch, piece = inputs.shape
    total = micro * batch
    width = weights.shape[-1]
    depth = weights.shape[1] * weights.shape[3]
    count = total // CHUNK_ROWS
    rows = CHUNK_ROWS
    x = inputs.reshape(total, piece)
    w = weights.reshape(depth, width)
    blocks = width // piece
    dma = pltpu.SemaphoreType.DMA
    out = pl.pallas_call(
        functools.partial(kernel, count),
        out_shape=jax.ShapeDtypeStruct((total, piece), F32),
        in_specs=[
            pl.BlockSpec(memory_space=pl.ANY),
            pl.BlockSpec(memory_space=pl.ANY),
            pl.BlockSpec(memory_space=pltpu.VMEM),
        ],
        out_specs=pl.BlockSpec(memory_space=pltpu.VMEM),
        scratch_shapes=[
            pltpu.VMEM((blocks, depth, piece), F32),
            pltpu.VMEM((blocks, depth, piece), BF16),
            pltpu.VMEM((blocks, depth, piece), BF16),
            pltpu.VMEM((2 * rows, depth), BF16),
            pltpu.VMEM((8, total, piece), F32),
            pltpu.VMEM((8, total, piece), F32),
            pltpu.VMEM((count, 2, rows, piece), F32),
            pltpu.VMEM((count, 2, rows, piece), F32),
            pltpu.VMEM((count, 2, 2, rows, piece), F32),
            pltpu.VMEM((count, 2, 2, rows, piece), F32),
            pltpu.VMEM((count, 2, rows, piece), F32),
            pltpu.VMEM((count, rows, piece), F32),
            pltpu.VMEM((count, rows, piece), F32),
            pltpu.VMEM((total, piece), F32),
            pltpu.VMEM((count, 8, 8, 128), F32),
            pltpu.VMEM((count, 8, 8, 128), F32),
            pltpu.VMEM((count, 8, 128), F32),
            pltpu.VMEM((count, 8, 128), F32),
            dma((8,)),
            dma(()),
            dma((2, count, 9)),
            dma((2, count, 9)),
            dma((count, 2)),
            dma((count, 2)),
            dma((count, 4)),
            dma((count, 4)),
            dma((count,)),
            dma((count,)),
            dma((count,)),
            dma((count,)),
            dma((count,)),
            dma((count,)),
            dma((count,)),
            dma((count,)),
            dma((count,)),
            dma((count,)),
        ],
        compiler_params=pltpu.CompilerParams(
            collective_id=0, has_side_effects=True, vmem_limit_bytes=62 * 1024 * 1024
        ),
    )(x, w, norm_gain)
    return out.reshape(1, micro, batch, piece)


def solution(mesh):
    placed = (
        P(None, None, ("row", "col")),
        P("section", None, "col", None, "row"),
        P("section", ("row", "col")),
    )
    return jax.shard_map(
        shards,
        mesh=mesh,
        in_specs=placed,
        out_specs=P("section", None, None, ("row", "col")),
        check_vma=False,
    )
```

```python
import functools

import jax
import jax.numpy as jnp
from jax import lax
from jax.experimental import pallas as pl
from jax.experimental.pallas import tpu as pltpu
from jax.sharding import PartitionSpec as P

MESH = pl.DeviceIdType.MESH
F32 = jnp.float32
BF16 = jnp.bfloat16
SIZES = (96, 96, 96, 96)


def kernel(
    x_ref, w_ref, gain_ref, out_ref,
    wf, w1, w2, xd, g1, g2, p1s, p1r, p2s, p2r, own, zs, zr, yg, sa, sb, st, sr, ob,
    wsem, xsem, osem, ag_s, ag_r, p1_ss, p1_rs, p2_ss, p2_rs, z_ss, z_rs, t_ss, t_rs, st_ss, st_rs,
    sa_ss, sa_rs, sb_ss, sb_rs,
):
    count = len(SIZES)
    starts = [sum(SIZES[:c]) for c in range(count)]
    sec = lax.axis_index("section")
    r = lax.axis_index("row")
    q = lax.axis_index("col")
    piece = out_ref.shape[1]
    features = piece * 64
    y = q // 2
    z = q % 2
    xp, xm, x2 = (r + 2) % 8, (r + 6) % 8, (r + 4) % 8
    mate = r + 1 - 2 * (r % 2)
    yp, ym = (q + 2) % 8, (q + 6) % 8
    zmate = q + 1 - 2 * z
    to_xp, to_xm, to_mate = {"row": xp}, {"row": xm}, {"row": mate}
    to_yp, to_ym, to_z = {"col": yp}, {"col": ym}, {"col": zmate}
    to_next = {"section": 1 - sec}

    def named(f):
        def call(*a):
            tag = "_".join(str(v) for v in a if isinstance(v, int))
            with jax.named_scope(f"{f.__name__}#a={tag}"):
                return f(*a)

        return call

    def cp(src, dst, ss, rs, dev):
        return pltpu.make_async_remote_copy(
            src_ref=src, dst_ref=dst, send_sem=ss, recv_sem=rs, device_id=dev, device_id_type=MESH
        )

    def got(ref, ss, rs):
        return cp(ref, ref, ss, rs, to_mate)

    def block(off):
        return (y + off) % 4

    def rs(c):
        return pl.ds(starts[c], SIZES[c])

    def ra(c):
        return pl.ds(starts[c], SIZES[c] // 2)

    def rb(c):
        return pl.ds(starts[c] + SIZES[c] // 2, SIZES[c] // 2)

    offs = (2, 1, 3, 0)

    def wcopy(k):
        nb = block(offs[k // 2]) * 2 + k % 2
        cols = pl.ds(pl.multiple_of(nb * piece, piece), piece)
        return pltpu.make_async_copy(w_ref.at[:, cols], wf.at[nb], wsem.at[k]), nb

    xcopy = pltpu.make_async_copy(x_ref, g1.at[r], xsem)
    xcopy.start()
    peers = [{"row": (r + d) % 8} for d in range(1, 8)]
    peers += [{"col": (q + d) % 8} for d in range(1, 8)]
    peers += [to_next]
    barrier = pltpu.get_barrier_semaphore()
    for dev in peers:
        pl.semaphore_signal(barrier, inc=1, device_id=dev, device_id_type=MESH)
    with jax.named_scope("xwait"):
        xcopy.wait()
    for k in range(8):
        wcopy(k)[0].start()
    with jax.named_scope("barrier"):
        pl.semaphore_wait(barrier, len(peers))

    def ag(g, n, c, j):
        piece_of, part = (
            (r, rs(c)), (r, rs(c)), (r, rs(c)), (xm, ra(c)), (xp, rb(c)),
            (xm, rs(c)), (xp, rs(c)), (x2, ra(c)), (x2, rb(c)),
        )[j]
        dev = (to_xp, to_xm, to_mate, to_xp, to_xm, to_mate, to_mate, to_mate, to_mate)[j]
        slot = (0, 1, 4, 2, 3, 4, 4, 4, 4)[j]
        ref = g.at[piece_of, part, :]
        return cp(ref, ref, ag_s.at[n], ag_r.at[n, c, slot], dev)

    def ag_got(g, n, c, slot):
        piece_of, part = ((xm, rs(c)), (xp, rs(c)), (x2, ra(c)), (x2, rb(c)))[slot]
        got(g.at[piece_of, part, :], ag_s.at[n], ag_r.at[n, c, slot]).wait_recv()

    @named
    def ag1(g, n, c):
        for j in (0, 1, 2):
            ag(g, n, c, j).start()

    @named
    def ag2(g, n, c):
        ag_got(g, n, c, 0)
        ag(g, n, c, 3).start()
        ag(g, n, c, 5).start()
        ag_got(g, n, c, 1)
        ag(g, n, c, 4).start()
        ag(g, n, c, 6).start()

    @named
    def ag3(g, n, c):
        ag_got(g, n, c, 2)
        ag(g, n, c, 7).start()
        ag_got(g, n, c, 3)
        ag(g, n, c, 8).start()

    @named
    def ag4(g, n, c):
        got(g.at[pl.ds(0, 4), rs(c), :], ag_s.at[n], ag_r.at[n, c, 4]).wait_recv()

    @named
    def slice_weights(k):
        copy, nb = wcopy(k)
        copy.wait()

        def body(t, carry):
            rr = pl.ds(pl.multiple_of(t * 256, 256), 256)
            v = wf[nb, rr, :]
            a = v.astype(BF16)
            w1[nb, rr, :] = a
            w2[nb, rr, :] = (v - a.astype(F32)).astype(BF16)
            return carry

        lax.fori_loop(0, 8, body, 0)

    def as_row(v):
        rows = v.shape[0]
        h = v[:, :128] + v[:, 128:]
        if rows < 128:
            h = jnp.concatenate([h, jnp.zeros((128 - rows, 128), F32)], axis=0)
        t = jnp.sum(jnp.transpose(h), axis=0, keepdims=True)
        return jnp.broadcast_to(t, (8, 128))

    def scale_of(total, rows):
        inv = lax.rsqrt(total / features + 1e-06)
        t = jnp.transpose(jnp.broadcast_to(inv[:1], (128, 128)))[:rows]
        return jnp.concatenate([t, t], axis=1)

    def split_into(i, v):
        rows = v.shape[0]
        a = v.astype(BF16)
        cols = pl.ds(i * piece, piece)
        xd[0:rows, cols] = a
        xd[rows : 2 * rows, cols] = (v - a.astype(F32)).astype(BF16)

    @named
    def prep0(c):
        for i in range(8):
            split_into(i, g1[i, rs(c), :])

    @named
    def prep1(c):
        scale = scale_of(sr[c], SIZES[c])
        for i in range(8):
            split_into(i, g1[i, rs(c), :] + g2[i, rs(c), :] * scale)

    @named
    def mm(c, off):
        rows = SIZES[c]
        base = block(off) * 2

        def body(zz, carry):
            a = jnp.dot(xd[0 : 2 * rows, :], w1[base + zz], preferred_element_type=F32)
            b = jnp.dot(xd[0:rows, :], w2[base + zz], preferred_element_type=F32)
            v = a[:rows] + a[rows:] + b
            if off == 2:
                p1s[zz, rs(c), :] = v
            elif off == 0:
                own[zz, rs(c), :] = v
            else:
                p2s[off // 2, zz, rs(c), :] = v
            return carry

        lax.fori_loop(0, 2, body, 0)
        if off == 2:
            p1(c, 0).start()
            p1(c, 1).start()
        elif off:
            p2(c, off // 2).start()

    def p1(c, j):
        part, dev = ((ra(c), to_yp), (rb(c), to_ym))[j]
        return cp(p1s.at[:, part, :], p1r.at[:, part, :], p1_ss, p1_rs.at[c, j], dev)

    def p2(c, j):
        d, part, dev = ((0, rb(c), to_yp), (1, ra(c), to_ym), (0, ra(c), to_yp), (1, rb(c), to_ym))[j]
        return cp(p2s.at[d, :, part, :], p2r.at[d, :, part, :], p2_ss, p2_rs.at[c], dev)

    @named
    def f1(c):
        for j, part in ((0, ra(c)), (1, rb(c))):
            got(p1r.at[:, part, :], p1_ss, p1_rs.at[c, j]).wait_recv()
            p2s[j, :, part, :] = p2s[j, :, part, :] + p1r[:, part, :]
            p2(c, 2 + j).start()

    def zcopy(c):
        return cp(zs.at[rs(c), :], zr.at[rs(c), :], z_ss, z_rs.at[c], to_z)

    @named
    def f2(c):
        got(p2r.at[:, :, rs(c), :], p2_ss, p2_rs.at[c]).wait_recv()
        zs[rs(c), :] = own[1 - z, rs(c), :] + p2r[0, 1 - z, rs(c), :] + p2r[1, 1 - z, rs(c), :]
        zcopy(c).start()
        own[z, rs(c), :] = own[z, rs(c), :] + p2r[0, z, rs(c), :] + p2r[1, z, rs(c), :]

    def tcopy(c):
        return cp(yg.at[rs(c), :], g2.at[r, rs(c), :], t_ss, t_rs.at[c], to_next)

    def sacopy(c, d):
        return cp(sa.at[c, r], sa.at[c, r], sa_ss, sa_rs.at[c], {"row": (r + d) % 8})

    def sbcopy(c, d):
        return cp(sb.at[c, q], sb.at[c, q], sb_ss, sb_rs.at[c], {"col": (q + d) % 8})

    def stcopy(c):
        return cp(st.at[c], sr.at[c], st_ss, st_rs.at[c], to_next)

    @named
    def f3(c, send):
        zcopy(c).wait_recv()
        v = jax.nn.gelu(own[z, rs(c), :] + zr[rs(c), :], approximate=True)
        yg[rs(c), :] = v * gain_ref[...]
        if send:
            tcopy(c).start()
        sa[c, r] = as_row(v * v)
        for d in range(1, 8):
            sacopy(c, d).start()

    @named
    def f4(c):
        got(sa.at[c, pl.ds(0, 7)], sa_ss, sa_rs.at[c]).wait_recv()
        t = sa[c, 0]
        for i in range(1, 8):
            t = t + sa[c, i]
        sb[c, q] = t
        for d in range(1, 8):
            sbcopy(c, d).start()

    def ocopy(c):
        return pltpu.make_async_copy(ob.at[rs(c), :], out_ref.at[rs(c), :], osem)

    @named
    def f5(c, send):
        got(sb.at[c, pl.ds(0, 7)], sb_ss, sb_rs.at[c]).wait_recv()
        t = sb[c, 0]
        for i in range(1, 8):
            t = t + sb[c, i]
        if send:
            st[c] = t
            stcopy(c).start()
        ob[rs(c), :] = yg[rs(c), :] * scale_of(t, SIZES[c])
        ocopy(c).start()

    def when(c):
        return 0 <= c < count

    @pl.when(sec == 0)
    def _():
        ag1(g1, 0, 0)
        for k in range(4):
            slice_weights(k)
        ag2(g1, 0, 0)
        ag1(g1, 0, 1)
        for k in range(4, 8):
            slice_weights(k)
        ag3(g1, 0, 0)
        ag2(g1, 0, 1)
        if when(2):
            ag1(g1, 0, 2)
        for c in range(count):
            ag4(g1, 0, c)
            prep0(c)
            mm(c, 2)
            mm(c, 1)
            if when(c - 2):
                f3(c - 2, True)
            mm(c, 3)
            if when(c + 1):
                ag3(g1, 0, c + 1)
            if when(c + 2):
                ag2(g1, 0, c + 2)
            if when(c + 3):
                ag1(g1, 0, c + 3)
            mm(c, 0)
            if when(c - 1):
                f2(c - 1)
            if when(c - 3):
                f5(c - 3, True)
            f1(c)
            if when(c - 2):
                f4(c - 2)
        n = count - 1
        f3(n - 1, True)
        f2(n)
        f5(n - 2, True)
        f4(n - 1)
        f3(n, True)
        f5(n - 1, True)
        f4(n)
        f5(n, True)
        got(yg, t_ss, t_rs.at[0]).wait_send()
        got(st, st_ss, st_rs.at[0]).wait_send()

    @pl.when(sec == 1)
    def _():
        ag1(g1, 0, 0)
        for k in range(4):
            slice_weights(k)
        ag2(g1, 0, 0)
        for k in range(4, 8):
            slice_weights(k)
        for c in range(count):
            if when(c + 1):
                ag1(g1, 0, c + 1)
            ag3(g1, 0, c)
            if when(c + 1):
                ag2(g1, 0, c + 1)
        for c in range(count):
            ag4(g1, 0, c)

        @named
        def start(c):
            got(g2.at[r, rs(c), :], t_ss, t_rs.at[c]).wait_recv()
            ag1(g2, 1, c)

        start(0)
        ag2(g2, 1, 0)
        if when(1):
            start(1)
        ag3(g2, 1, 0)
        for c in range(count):
            ag4(g2, 1, c)
            with jax.named_scope(f"stwait#a={c}"):
                got(sr.at[c], st_ss, st_rs.at[c]).wait_recv()
            prep1(c)
            mm(c, 2)
            if when(c + 1):
                ag2(g2, 1, c + 1)
            mm(c, 1)
            if when(c - 2):
                f3(c - 2, False)
            mm(c, 3)
            if when(c + 2):
                start(c + 2)
            mm(c, 0)
            if when(c - 1):
                f2(c - 1)
            if when(c + 1):
                ag3(g2, 1, c + 1)
            if when(c - 3):
                f5(c - 3, False)
            f1(c)
            if when(c - 2):
                f4(c - 2)
        n = count - 1
        f3(n - 1, False)
        f2(n)
        f5(n - 2, False)
        f4(n - 1)
        f3(n, False)
        f5(n - 1, False)
        f4(n)
        f5(n, False)
        got(g2.at[pl.ds(0, 7)], ag_s.at[1], ag_r.at[1, 0, 0]).wait_send()

    got(g1.at[pl.ds(0, 7)], ag_s.at[0], ag_r.at[0, 0, 0]).wait_send()
    got(p1s, p1_ss, p1_rs.at[0, 0]).wait_send()
    got(p2s, p2_ss, p2_rs.at[0]).wait_send()
    got(zs, z_ss, z_rs.at[0]).wait_send()
    got(sa.at[:, pl.ds(0, 7)], sa_ss, sa_rs.at[0]).wait_send()
    got(sb.at[:, pl.ds(0, 7)], sb_ss, sb_rs.at[0]).wait_send()
    pltpu.make_async_copy(ob, out_ref, osem).wait()


def shards(inputs, weights, norm_gain):
    micro, batch, piece = inputs.shape
    total = micro * batch
    width = weights.shape[-1]
    depth = weights.shape[1] * weights.shape[3]
    count = len(SIZES)
    rows = max(SIZES)
    x = inputs.reshape(total, piece)
    w = weights.reshape(depth, width)
    blocks = width // piece
    dma = pltpu.SemaphoreType.DMA
    out = pl.pallas_call(
        kernel,
        out_shape=jax.ShapeDtypeStruct((total, piece), F32),
        in_specs=[
            pl.BlockSpec(memory_space=pl.ANY),
            pl.BlockSpec(memory_space=pl.ANY),
            pl.BlockSpec(memory_space=pltpu.VMEM),
        ],
        out_specs=pl.BlockSpec(memory_space=pl.ANY),
        scratch_shapes=[
            pltpu.VMEM((blocks, depth, piece), F32),
            pltpu.VMEM((blocks, depth, piece), BF16),
            pltpu.VMEM((blocks, depth, piece), BF16),
            pltpu.VMEM((2 * rows, depth), BF16),
            pltpu.VMEM((8, total, piece), F32),
            pltpu.VMEM((8, total, piece), F32),
            pltpu.VMEM((2, total, piece), F32),
            pltpu.VMEM((2, total, piece), F32),
            pltpu.VMEM((2, 2, total, piece), F32),
            pltpu.VMEM((2, 2, total, piece), F32),
            pltpu.VMEM((2, total, piece), F32),
            pltpu.VMEM((total, piece), F32),
            pltpu.VMEM((total, piece), F32),
            pltpu.VMEM((total, piece), F32),
            pltpu.VMEM((count, 8, 8, 128), F32),
            pltpu.VMEM((count, 8, 8, 128), F32),
            pltpu.VMEM((count, 8, 128), F32),
            pltpu.VMEM((count, 8, 128), F32),
            pltpu.VMEM((total, piece), F32),
            dma((8,)),
            dma(()),
            dma(()),
            dma((2,)),
            dma((2, count, 5)),
            dma(()),
            dma((count, 2)),
            dma(()),
            dma((count,)),
            dma(()),
            dma((count,)),
            dma(()),
            dma((count,)),
            dma(()),
            dma((count,)),
            dma(()),
            dma((count,)),
            dma(()),
            dma((count,)),
        ],
        compiler_params=pltpu.CompilerParams(
            collective_id=0, has_side_effects=True, vmem_limit_bytes=62 * 1024 * 1024
        ),
    )(x, w, norm_gain)
    return out.reshape(1, micro, batch, piece)


def solution(mesh):
    placed = (
        P(None, None, ("row", "col")),
        P("section", None, "col", None, "row"),
        P("section", ("row", "col")),
    )
    return jax.shard_map(
        shards,
        mesh=mesh,
        in_specs=placed,
        out_specs=P("section", None, None, ("row", "col")),
        check_vma=False,
    )
```

```python
import functools

import jax
import jax.numpy as jnp
from jax import lax
from jax.experimental import pallas as pl
from jax.experimental.pallas import tpu as pltpu
from jax.sharding import PartitionSpec as P

MESH = pl.DeviceIdType.MESH
F32 = jnp.float32
BF16 = jnp.bfloat16
SIZES = (96, 96, 96, 96)
WIDE = (128, 128, 128)


def kernel(
    x_ref, w_ref, gain_ref, out_ref,
    wf, w1, w2, xd, g1, g2, p1s, p1r, p2s, p2r, own, zs, zr, yg, sa, sb, st, sr, ob, pre, scv,
    wsem, xsem, osem, ag_s, ag_r, p1_ss, p1_rs, p2_ss, p2_rs, z_ss, z_rs, t_ss, t_rs, st_ss, st_rs,
    sa_ss, sa_rs, sb_ss, sb_rs,
):
    count = len(SIZES)
    lens = SIZES + WIDE
    starts = [sum(SIZES[:c]) for c in range(count)] + [sum(WIDE[:c]) for c in range(len(WIDE))]
    sec = lax.axis_index("section")
    r = lax.axis_index("row")
    q = lax.axis_index("col")
    piece = out_ref.shape[1]
    features = piece * 64
    y = q // 2
    z = q % 2
    xp, xm, x2 = (r + 2) % 8, (r + 6) % 8, (r + 4) % 8
    mate = r + 1 - 2 * (r % 2)
    yp, ym = (q + 2) % 8, (q + 6) % 8
    zmate = q + 1 - 2 * z
    to_xp, to_xm, to_mate = {"row": xp}, {"row": xm}, {"row": mate}
    to_yp, to_ym, to_z = {"col": yp}, {"col": ym}, {"col": zmate}
    to_next = {"section": 1 - sec}

    def named(f):
        def call(*a):
            tag = "_".join(str(v) for v in a if isinstance(v, int))
            with jax.named_scope(f"{f.__name__}#a={tag}"):
                return f(*a)

        return call

    def cp(src, dst, ss, rs, dev):
        return pltpu.make_async_remote_copy(
            src_ref=src, dst_ref=dst, send_sem=ss, recv_sem=rs, device_id=dev, device_id_type=MESH
        )

    def got(ref, ss, rs):
        return cp(ref, ref, ss, rs, to_mate)

    def block(off):
        return (y + off) % 4

    def rs(c):
        return pl.ds(starts[c], lens[c])

    def ra(c):
        return pl.ds(starts[c], lens[c] // 2)

    def rb(c):
        return pl.ds(starts[c] + lens[c] // 2, lens[c] // 2)

    offs = (2, 1, 3, 0)

    def wcopy(k):
        nb = block(offs[k // 2]) * 2 + k % 2
        cols = pl.ds(pl.multiple_of(nb * piece, piece), piece)
        return pltpu.make_async_copy(w_ref.at[:, cols], wf.at[nb], wsem.at[k]), nb

    xcopy = pltpu.make_async_copy(x_ref, g1.at[r], xsem)
    xcopy.start()
    peers = [{"row": (r + d) % 8} for d in range(1, 8)]
    peers += [{"col": (q + d) % 8} for d in range(1, 8)]
    peers += [to_next]
    barrier = pltpu.get_barrier_semaphore()
    for dev in peers:
        pl.semaphore_signal(barrier, inc=1, device_id=dev, device_id_type=MESH)
    with jax.named_scope("xwait"):
        xcopy.wait()
    for k in range(8):
        wcopy(k)[0].start()
    with jax.named_scope("barrier"):
        pl.semaphore_wait(barrier, len(peers))

    def ag(g, n, c, piece_of, part, dev, slot):
        ref = g.at[piece_of, part, :]
        cp(ref, ref, ag_s.at[n], ag_r.at[n, c % count, slot], dev).start()

    def ag_got(g, n, c, slot):
        piece_of, part = (
            (xm, ra(c)), (xp, rb(c)), (xm, rb(c)), (xp, ra(c)), (x2, ra(c)), (x2, rb(c)),
            (pl.ds(0, 3), rs(c)), (0, rs(c)),
        )[slot]
        got(g.at[piece_of, part, :], ag_s.at[n], ag_r.at[n, c % count, slot]).wait_recv()

    @named
    def ag1(g, n, c):
        ag(g, n, c, r, ra(c), to_xp, 0)
        ag(g, n, c, r, rb(c), to_xm, 1)
        ag(g, n, c, r, rb(c), to_xp, 2)
        ag(g, n, c, r, ra(c), to_xm, 3)
        ag(g, n, c, r, rs(c), to_mate, 6)

    @named
    def ag2(g, n, c):
        ag_got(g, n, c, 0)
        ag(g, n, c, xm, ra(c), to_xp, 4)
        ag(g, n, c, xm, ra(c), to_mate, 6)
        ag_got(g, n, c, 1)
        ag(g, n, c, xp, rb(c), to_xm, 5)
        ag(g, n, c, xp, rb(c), to_mate, 6)

    @named
    def ag2b(g, n, c):
        ag_got(g, n, c, 2)
        ag(g, n, c, xm, rb(c), to_mate, 6)
        ag_got(g, n, c, 3)
        ag(g, n, c, xp, ra(c), to_mate, 6)

    @named
    def ag3(g, n, c):
        ag_got(g, n, c, 4)
        ag(g, n, c, x2, ra(c), to_mate, 7)
        ag_got(g, n, c, 5)
        ag(g, n, c, x2, rb(c), to_mate, 7)

    @named
    def near_in(g, n, c):
        ag_got(g, n, c, 6)

    @named
    def far_in(g, n, c):
        ag_got(g, n, c, 7)

    def piece_at(t):
        return ((r // 2 + 3) * 2 + t) % 8

    @named
    def slice_weights(k):
        copy, nb = wcopy(k)
        copy.wait()

        def body(t, carry):
            src = pl.ds(pl.multiple_of(piece_at(t) * piece, piece), piece)
            dst = pl.ds(pl.multiple_of(t * piece, piece), piece)
            v = wf[nb, src, :]
            a = v.astype(BF16)
            w1[nb, dst, :] = a
            w2[nb, dst, :] = (v - a.astype(F32)).astype(BF16)
            return carry

        lax.fori_loop(0, 8, body, 0)

    def as_row(v):
        rows = v.shape[0]
        h = v[:, :128] + v[:, 128:]
        if rows < 128:
            h = jnp.concatenate([h, jnp.zeros((128 - rows, 128), F32)], axis=0)
        t = jnp.sum(jnp.transpose(h), axis=0, keepdims=True)
        return jnp.broadcast_to(t, (8, 128))

    def scale_of(total, rows):
        inv = lax.rsqrt(total / features + 1e-06)
        t = jnp.transpose(jnp.broadcast_to(inv[:1], (128, 128)))[:rows]
        return jnp.concatenate([t, t], axis=1)

    NEAR, FAR, ALL = (0, 6), (6, 8), (0, 8)

    @named
    def prep(c, g, span):
        rows = lens[c]
        for t in range(*span):
            v = g[piece_at(t), rs(c), :]
            a = v.astype(BF16)
            cols = pl.ds(t * piece, piece)
            xd[0:rows, cols] = a
            xd[rows : 2 * rows, cols] = (v - a.astype(F32)).astype(BF16)

    def mul(c, off, span, into, plus=False, ahead=False):
        rows = lens[c]
        base = block(off) * 2
        k = pl.ds(span[0] * piece, (span[1] - span[0]) * piece)

        def body(zz, carry):
            a = jnp.dot(xd[0 : 2 * rows, k], w1[base + zz, k, :], preferred_element_type=F32)
            b = jnp.dot(xd[0:rows, k], w2[base + zz, k, :], preferred_element_type=F32)
            v = a[:rows] + a[rows:] + b
            at = (pre if into == "pre" else p1s if off == 2 else own if off == 0 else p2s)
            where = (
                (off, zz, rs(c)) if into == "pre" else (zz, rs(c)) if off in (0, 2) else (off // 2, zz, rs(c))
            )
            if plus:
                v = v + at[where]
            if ahead:
                v = v * scv[0:rows, :] + pre[off, zz, rs(c), :]
            at[where] = v
            return carry

        lax.fori_loop(0, 2, body, 0)
        if into == "send":
            if off == 2:
                p1(c, 0).start()
                p1(c, 1).start()
            elif off:
                p2(c, off // 2).start()

    @named
    def near(c, off):
        mul(c, off, NEAR, "hold")

    @named
    def far(c, off, ahead):
        mul(c, off, FAR, "send", plus=True, ahead=ahead)

    @named
    def mm(c, off, ahead=False):
        mul(c, off, ALL, "send", ahead=ahead)

    @named
    def early(c, off):
        mul(c, off, ALL, "pre")

    def p1(c, j):
        part, dev = ((ra(c), to_yp), (rb(c), to_ym))[j]
        return cp(p1s.at[:, part, :], p1r.at[:, part, :], p1_ss, p1_rs.at[c, j], dev)

    def p2(c, j):
        d, part, dev = ((0, rb(c), to_yp), (1, ra(c), to_ym), (0, ra(c), to_yp), (1, rb(c), to_ym))[j]
        return cp(p2s.at[d, :, part, :], p2r.at[d, :, part, :], p2_ss, p2_rs.at[c], dev)

    @named
    def f1(c):
        for j, part in ((0, ra(c)), (1, rb(c))):
            got(p1r.at[:, part, :], p1_ss, p1_rs.at[c, j]).wait_recv()
            p2s[j, :, part, :] = p2s[j, :, part, :] + p1r[:, part, :]
            p2(c, 2 + j).start()

    def zcopy(c):
        return cp(zs.at[rs(c), :], zr.at[rs(c), :], z_ss, z_rs.at[c], to_z)

    @named
    def f2(c):
        got(p2r.at[:, :, rs(c), :], p2_ss, p2_rs.at[c]).wait_recv()
        zs[rs(c), :] = own[1 - z, rs(c), :] + p2r[0, 1 - z, rs(c), :] + p2r[1, 1 - z, rs(c), :]
        zcopy(c).start()
        own[z, rs(c), :] = own[z, rs(c), :] + p2r[0, z, rs(c), :] + p2r[1, z, rs(c), :]

    def tcopy(c):
        return cp(yg.at[rs(c), :], g2.at[r, rs(c), :], t_ss, t_rs.at[c], to_next)

    def sacopy(c, d):
        return cp(sa.at[c, r], sa.at[c, r], sa_ss, sa_rs.at[c], {"row": (r + d) % 8})

    def sbcopy(c, d):
        return cp(sb.at[c, q], sb.at[c, q], sb_ss, sb_rs.at[c], {"col": (q + d) % 8})

    def stcopy(c):
        return cp(st.at[c], sr.at[c], st_ss, st_rs.at[c], to_next)

    @named
    def f3(c, send):
        zcopy(c).wait_recv()
        v = jax.nn.gelu(own[z, rs(c), :] + zr[rs(c), :], approximate=True)
        yg[rs(c), :] = v * gain_ref[...]
        if send:
            tcopy(c).start()
        sa[c, r] = as_row(v * v)
        for d in range(1, 8):
            sacopy(c, d).start()

    @named
    def f4(c):
        got(sa.at[c, pl.ds(0, 7)], sa_ss, sa_rs.at[c]).wait_recv()
        t = sa[c, 0]
        for i in range(1, 8):
            t = t + sa[c, i]
        sb[c, q] = t
        for d in range(1, 8):
            sbcopy(c, d).start()

    def ocopy(c):
        return pltpu.make_async_copy(ob.at[rs(c), :], out_ref.at[rs(c), :], osem)

    @named
    def f5(c, send):
        got(sb.at[c, pl.ds(0, 7)], sb_ss, sb_rs.at[c]).wait_recv()
        t = sb[c, 0]
        for i in range(1, 8):
            t = t + sb[c, i]
        if send:
            st[c] = t
            stcopy(c).start()
        ob[rs(c), :] = yg[rs(c), :] * scale_of(t, SIZES[c])
        ocopy(c).start()

    def when(c):
        return 0 <= c < count

    @pl.when(sec == 0)
    def _():
        ag1(g1, 0, 0)
        for k in range(4):
            slice_weights(k)
        ag2(g1, 0, 0)
        slice_weights(4)
        slice_weights(5)
        ag2b(g1, 0, 0)
        if when(1):
            ag1(g1, 0, 1)
        slice_weights(6)
        slice_weights(7)
        near_in(g1, 0, 0)
        prep(0, g1, NEAR)
        near(0, 2)
        ag3(g1, 0, 0)
        near(0, 1)
        far_in(g1, 0, 0)
        prep(0, g1, FAR)
        far(0, 2, False)
        far(0, 1, False)
        if when(1):
            ag2(g1, 0, 1)
        mm(0, 3)
        if when(1):
            ag2b(g1, 0, 1)
        if when(2):
            ag1(g1, 0, 2)
        mm(0, 0)
        if when(1):
            ag3(g1, 0, 1)
        f1(0)
        for c in range(1, count):
            near_in(g1, 0, c)
            far_in(g1, 0, c)
            prep(c, g1, ALL)
            mm(c, 2)
            if when(c + 1):
                ag2(g1, 0, c + 1)
                ag2b(g1, 0, c + 1)
            if when(c + 2):
                ag1(g1, 0, c + 2)
            if when(c - 2):
                f3(c - 2, True)
            mm(c, 1)
            if when(c - 3):
                f5(c - 3, True)
            mm(c, 3)
            f2(c - 1)
            mm(c, 0)
            if when(c + 1):
                ag3(g1, 0, c + 1)
            if when(c - 2):
                f4(c - 2)
            f1(c)
        n = count - 1
        f3(n - 1, True)
        f2(n)
        f5(n - 2, True)
        f4(n - 1)
        f3(n, True)
        f5(n - 1, True)
        f4(n)
        f5(n, True)
        got(yg, t_ss, t_rs.at[0]).wait_send()
        got(st, st_ss, st_rs.at[0]).wait_send()

    @pl.when(sec == 1)
    def _():
        wide = range(count, count + len(WIDE))
        ag1(g1, 0, wide[0])
        for k in range(4):
            slice_weights(k)
        ag2(g1, 0, wide[0])
        for k in range(4, 8):
            slice_weights(k)
        ag2b(g1, 0, wide[0])
        ag1(g1, 0, wide[1])
        ag3(g1, 0, wide[0])
        for c in wide:
            near_in(g1, 0, c)
            far_in(g1, 0, c)
            prep(c, g1, ALL)
            early(c, 2)
            if c + 1 in wide:
                ag2(g1, 0, c + 1)
            early(c, 1)
            if c + 1 in wide:
                ag2b(g1, 0, c + 1)
            if c + 2 in wide:
                ag1(g1, 0, c + 2)
            early(c, 3)
            if c + 1 in wide:
                ag3(g1, 0, c + 1)
            early(c, 0)

        @named
        def start(c):
            got(g2.at[r, rs(c), :], t_ss, t_rs.at[c]).wait_recv()
            ag1(g2, 1, c)

        start(0)
        ag2(g2, 1, 0)
        ag2b(g2, 1, 0)
        for c in range(count):
            if when(c + 1):
                start(c + 1)
            near_in(g2, 1, c)
            prep(c, g2, NEAR)
            near(c, 2)
            ag3(g2, 1, c)
            if when(c - 1):
                f1(c - 1)
            near(c, 1)
            far_in(g2, 1, c)
            with jax.named_scope(f"stwait#a={c}"):
                got(sr.at[c], st_ss, st_rs.at[c]).wait_recv()
            scv[0 : SIZES[c], :] = scale_of(sr[c], SIZES[c])
            prep(c, g2, FAR)
            far(c, 2, True)
            if when(c + 1):
                ag2(g2, 1, c + 1)
            far(c, 1, True)
            if when(c + 1):
                ag2b(g2, 1, c + 1)
            mm(c, 3, True)
            if when(c - 1):
                f2(c - 1)
            mm(c, 0, True)
            if when(c - 2):
                f3(c - 2, False)
            if when(c - 3):
                f4(c - 3)
        n = count - 1
        f1(n)
        f4(n - 2)
        f3(n - 1, False)
        f2(n)
        for c in range(n - 1):
            f5(c, False)
        f4(n - 1)
        f3(n, False)
        f5(n - 1, False)
        f4(n)
        f5(n, False)
        got(g2.at[pl.ds(0, 7)], ag_s.at[1], ag_r.at[1, 0, 0]).wait_send()

    got(g1.at[pl.ds(0, 7)], ag_s.at[0], ag_r.at[0, 0, 0]).wait_send()
    got(p1s, p1_ss, p1_rs.at[0, 0]).wait_send()
    got(p2s, p2_ss, p2_rs.at[0]).wait_send()
    got(zs, z_ss, z_rs.at[0]).wait_send()
    got(sa.at[:, pl.ds(0, 7)], sa_ss, sa_rs.at[0]).wait_send()
    got(sb.at[:, pl.ds(0, 7)], sb_ss, sb_rs.at[0]).wait_send()
    pltpu.make_async_copy(ob, out_ref, osem).wait()


def shards(inputs, weights, norm_gain):
    micro, batch, piece = inputs.shape
    total = micro * batch
    width = weights.shape[-1]
    depth = weights.shape[1] * weights.shape[3]
    count = len(SIZES)
    rows = max(SIZES + WIDE)
    x = inputs.reshape(total, piece)
    w = weights.reshape(depth, width)
    blocks = width // piece
    dma = pltpu.SemaphoreType.DMA
    out = pl.pallas_call(
        kernel,
        out_shape=jax.ShapeDtypeStruct((total, piece), F32),
        in_specs=[
            pl.BlockSpec(memory_space=pl.ANY),
            pl.BlockSpec(memory_space=pl.ANY),
            pl.BlockSpec(memory_space=pltpu.VMEM),
        ],
        out_specs=pl.BlockSpec(memory_space=pl.ANY),
        scratch_shapes=[
            pltpu.VMEM((blocks, depth, piece), F32),
            pltpu.VMEM((blocks, depth, piece), BF16),
            pltpu.VMEM((blocks, depth, piece), BF16),
            pltpu.VMEM((2 * rows, depth), BF16),
            pltpu.VMEM((8, total, piece), F32),
            pltpu.VMEM((8, total, piece), F32),
            pltpu.VMEM((2, total, piece), F32),
            pltpu.VMEM((2, total, piece), F32),
            pltpu.VMEM((2, 2, total, piece), F32),
            pltpu.VMEM((2, 2, total, piece), F32),
            pltpu.VMEM((2, total, piece), F32),
            pltpu.VMEM((total, piece), F32),
            pltpu.VMEM((total, piece), F32),
            pltpu.VMEM((total, piece), F32),
            pltpu.VMEM((count, 8, 8, 128), F32),
            pltpu.VMEM((count, 8, 8, 128), F32),
            pltpu.VMEM((count, 8, 128), F32),
            pltpu.VMEM((count, 8, 128), F32),
            pltpu.VMEM((total, piece), F32),
            pltpu.VMEM((4, 2, total, piece), F32),
            pltpu.VMEM((rows, piece), F32),
            dma((8,)),
            dma(()),
            dma(()),
            dma((2,)),
            dma((2, count, 8)),
            dma(()),
            dma((count, 2)),
            dma(()),
            dma((count,)),
            dma(()),
            dma((count,)),
            dma(()),
            dma((count,)),
            dma(()),
            dma((count,)),
            dma(()),
            dma((count,)),
            dma(()),
            dma((count,)),
        ],
        compiler_params=pltpu.CompilerParams(
            collective_id=0, has_side_effects=True, vmem_limit_bytes=62 * 1024 * 1024
        ),
    )(x, w, norm_gain)
    return out.reshape(1, micro, batch, piece)


def solution(mesh):
    placed = (
        P(None, None, ("row", "col")),
        P("section", None, "col", None, "row"),
        P("section", ("row", "col")),
    )
    return jax.shard_map(
        shards,
        mesh=mesh,
        in_specs=placed,
        out_specs=P("section", None, None, ("row", "col")),
        check_vma=False,
    )
```

```python
import functools

import jax
import jax.numpy as jnp
from jax import lax
from jax.experimental import pallas as pl
from jax.experimental.pallas import tpu as pltpu
from jax.sharding import PartitionSpec as P

MESH = pl.DeviceIdType.MESH
F32 = jnp.float32
BF16 = jnp.bfloat16
SIZES = (96, 96, 96, 96)
WIDE = (128, 128, 128)
SPLIT = (0, 1, 3)


def kernel(
    x_ref, w_ref, gain_ref, out_ref,
    wf, w1, w2, xd, g1, g2, p1s, p1r, p2s, p2r, own, zs, zr, yg, sa, sb, st, sr, ob, pre, scv,
    wsem, xsem, osem, ag_s, ag_r, p1_ss, p1_rs, p2_ss, p2_rs, z_ss, z_rs, t_ss, t_rs, st_ss, st_rs,
    sa_ss, sa_rs, sb_ss, sb_rs,
):
    count = len(SIZES)
    lens = SIZES + WIDE
    starts = [sum(SIZES[:c]) for c in range(count)] + [sum(WIDE[:c]) for c in range(len(WIDE))]
    sec = lax.axis_index("section")
    r = lax.axis_index("row")
    q = lax.axis_index("col")
    piece = out_ref.shape[1]
    features = piece * 64
    y = q // 2
    z = q % 2
    xp, xm, x2 = (r + 2) % 8, (r + 6) % 8, (r + 4) % 8
    mate = r + 1 - 2 * (r % 2)
    yp, ym = (q + 2) % 8, (q + 6) % 8
    zmate = q + 1 - 2 * z
    to_xp, to_xm, to_mate = {"row": xp}, {"row": xm}, {"row": mate}
    to_yp, to_ym, to_z = {"col": yp}, {"col": ym}, {"col": zmate}
    to_next = {"section": 1 - sec}

    def named(f):
        def call(*a):
            tag = "_".join(str(v) for v in a if isinstance(v, int))
            with jax.named_scope(f"{f.__name__}#a={tag}"):
                return f(*a)

        return call

    def cp(src, dst, ss, rs, dev):
        return pltpu.make_async_remote_copy(
            src_ref=src, dst_ref=dst, send_sem=ss, recv_sem=rs, device_id=dev, device_id_type=MESH
        )

    def got(ref, ss, rs):
        return cp(ref, ref, ss, rs, to_mate)

    def block(off):
        return (y + off) % 4

    def rs(c):
        return pl.ds(starts[c], lens[c])

    def ra(c):
        return pl.ds(starts[c], lens[c] // 2)

    def rb(c):
        return pl.ds(starts[c] + lens[c] // 2, lens[c] // 2)

    offs = (2, 1, 3, 0)

    def wcopy(k):
        nb = block(offs[k // 2]) * 2 + k % 2
        cols = pl.ds(pl.multiple_of(nb * piece, piece), piece)
        return pltpu.make_async_copy(w_ref.at[:, cols], wf.at[nb], wsem.at[k]), nb

    xcopy = pltpu.make_async_copy(x_ref, g1.at[r], xsem)
    xcopy.start()
    peers = [{"row": (r + d) % 8} for d in range(1, 8)]
    peers += [{"col": (q + d) % 8} for d in range(1, 8)]
    peers += [to_next]
    barrier = pltpu.get_barrier_semaphore()
    for dev in peers:
        pl.semaphore_signal(barrier, inc=1, device_id=dev, device_id_type=MESH)
    with jax.named_scope("xwait"):
        xcopy.wait()
    for k in range(8):
        wcopy(k)[0].start()
    with jax.named_scope("barrier"):
        pl.semaphore_wait(barrier, len(peers))

    def ag(g, n, c, piece_of, part, dev, slot):
        ref = g.at[piece_of, part, :]
        cp(ref, ref, ag_s.at[n], ag_r.at[n, c % count, slot], dev).start()

    def ag_got(g, n, c, slot):
        piece_of, part = (
            (xm, ra(c)), (xp, rb(c)), (xm, rb(c)), (xp, ra(c)), (x2, ra(c)), (x2, rb(c)),
            (pl.ds(0, 3), rs(c)), (0, rs(c)),
        )[slot]
        got(g.at[piece_of, part, :], ag_s.at[n], ag_r.at[n, c % count, slot]).wait_recv()

    @named
    def ag1(g, n, c):
        ag(g, n, c, r, ra(c), to_xp, 0)
        ag(g, n, c, r, rb(c), to_xm, 1)
        ag(g, n, c, r, rb(c), to_xp, 2)
        ag(g, n, c, r, ra(c), to_xm, 3)
        ag(g, n, c, r, rs(c), to_mate, 6)

    @named
    def ag2(g, n, c):
        ag_got(g, n, c, 0)
        ag(g, n, c, xm, ra(c), to_xp, 4)
        ag(g, n, c, xm, ra(c), to_mate, 6)
        ag_got(g, n, c, 1)
        ag(g, n, c, xp, rb(c), to_xm, 5)
        ag(g, n, c, xp, rb(c), to_mate, 6)

    @named
    def ag2b(g, n, c):
        ag_got(g, n, c, 2)
        ag(g, n, c, xm, rb(c), to_mate, 6)
        ag_got(g, n, c, 3)
        ag(g, n, c, xp, ra(c), to_mate, 6)

    @named
    def ag3(g, n, c):
        ag_got(g, n, c, 4)
        ag(g, n, c, x2, ra(c), to_mate, 7)
        ag_got(g, n, c, 5)
        ag(g, n, c, x2, rb(c), to_mate, 7)

    @named
    def near_in(g, n, c):
        ag_got(g, n, c, 6)

    @named
    def far_in(g, n, c):
        ag_got(g, n, c, 7)

    def piece_at(t):
        return ((r // 2 + 3) * 2 + t) % 8

    @named
    def slice_weights(k):
        copy, nb = wcopy(k)
        copy.wait()

        def body(t, carry):
            src = pl.ds(pl.multiple_of(piece_at(t) * piece, piece), piece)
            dst = pl.ds(pl.multiple_of(t * piece, piece), piece)
            v = wf[nb, src, :]
            a = v.astype(BF16)
            w1[nb, dst, :] = a
            w2[nb, dst, :] = (v - a.astype(F32)).astype(BF16)
            return carry

        lax.fori_loop(0, 8, body, 0)

    def as_row(v):
        rows = v.shape[0]
        h = v[:, :128] + v[:, 128:]
        if rows < 128:
            h = jnp.concatenate([h, jnp.zeros((128 - rows, 128), F32)], axis=0)
        return jnp.sum(jnp.transpose(h), axis=0, keepdims=True)

    def scale_of(total, rows):
        inv = lax.rsqrt(total / features + 1e-06)
        t = jnp.transpose(jnp.broadcast_to(inv, (128, 128)))[:rows]
        return jnp.concatenate([t, t], axis=1)

    NEAR, FAR, ALL = (0, 6), (6, 8), (0, 8)

    @named
    def prep(c, g, span):
        rows = lens[c]
        for t in range(*span):
            v = g[piece_at(t), rs(c), :]
            a = v.astype(BF16)
            cols = pl.ds(t * piece, piece)
            xd[0:rows, cols] = a
            xd[rows : 2 * rows, cols] = (v - a.astype(F32)).astype(BF16)

    def mul(c, off, span, into, plus=False, ahead=False):
        rows = lens[c]
        base = block(off) * 2
        k = pl.ds(span[0] * piece, (span[1] - span[0]) * piece)

        def body(zz, carry):
            a = jnp.dot(xd[0 : 2 * rows, k], w1[base + zz, k, :], preferred_element_type=F32)
            b = jnp.dot(xd[0:rows, k], w2[base + zz, k, :], preferred_element_type=F32)
            v = a[:rows] + a[rows:] + b
            at = (pre if into == "pre" else p1s if off == 2 else own if off == 0 else p2s)
            where = (
                (off, zz, rs(c)) if into == "pre" else (zz, rs(c)) if off in (0, 2) else (off // 2, zz, rs(c))
            )
            if plus:
                v = v + at[where]
            if ahead:
                v = v * scv[0:rows, :] + pre[off, zz, rs(c), :]
            at[where] = v
            return carry

        lax.fori_loop(0, 2, body, 0)
        if into == "send":
            if off == 2:
                p1(c, 0).start()
                p1(c, 1).start()
            elif off:
                p2(c, off // 2).start()

    @named
    def near(c, off):
        mul(c, off, NEAR, "hold")

    @named
    def far(c, off, ahead):
        mul(c, off, FAR, "send", plus=True, ahead=ahead)

    @named
    def mm(c, off, ahead=False):
        mul(c, off, ALL, "send", ahead=ahead)

    @named
    def early(c, off):
        mul(c, off, ALL, "pre")

    def p1(c, j):
        part, dev = ((ra(c), to_yp), (rb(c), to_ym))[j]
        return cp(p1s.at[:, part, :], p1r.at[:, part, :], p1_ss, p1_rs.at[c, j], dev)

    def p2(c, j):
        d, part, dev = ((0, rb(c), to_yp), (1, ra(c), to_ym), (0, ra(c), to_yp), (1, rb(c), to_ym))[j]
        return cp(p2s.at[d, :, part, :], p2r.at[d, :, part, :], p2_ss, p2_rs.at[c], dev)

    @named
    def f1(c):
        for j, part in ((0, ra(c)), (1, rb(c))):
            got(p1r.at[:, part, :], p1_ss, p1_rs.at[c, j]).wait_recv()
            p2s[j, :, part, :] = p2s[j, :, part, :] + p1r[:, part, :]
            p2(c, 2 + j).start()

    def zcopy(c):
        return cp(zs.at[rs(c), :], zr.at[rs(c), :], z_ss, z_rs.at[c], to_z)

    @named
    def f2(c):
        got(p2r.at[:, :, rs(c), :], p2_ss, p2_rs.at[c]).wait_recv()
        zs[rs(c), :] = own[1 - z, rs(c), :] + p2r[0, 1 - z, rs(c), :] + p2r[1, 1 - z, rs(c), :]
        zcopy(c).start()
        own[z, rs(c), :] = own[z, rs(c), :] + p2r[0, z, rs(c), :] + p2r[1, z, rs(c), :]

    def tcopy(c):
        return cp(yg.at[rs(c), :], g2.at[r, rs(c), :], t_ss, t_rs.at[c], to_next)

    def sacopy(c, d):
        return cp(sa.at[c, r], sa.at[c, r], sa_ss, sa_rs.at[c], {"row": (r + d) % 8})

    def sbcopy(c, d):
        return cp(sb.at[c, q], sb.at[c, q], sb_ss, sb_rs.at[c], {"col": (q + d) % 8})

    def stcopy(c):
        return cp(st.at[c], sr.at[c], st_ss, st_rs.at[c], to_next)

    @named
    def f3(c, send):
        zcopy(c).wait_recv()
        v = jax.nn.gelu(own[z, rs(c), :] + zr[rs(c), :], approximate=True)
        yg[rs(c), :] = v * gain_ref[...]
        if send:
            tcopy(c).start()
        sa[c, r] = as_row(v * v)
        for d in range(1, 8):
            sacopy(c, d).start()

    @named
    def f4(c):
        got(sa.at[c, pl.ds(0, 7)], sa_ss, sa_rs.at[c]).wait_recv()
        t = sa[c, 0]
        for i in range(1, 8):
            t = t + sa[c, i]
        sb[c, q] = t
        for d in range(1, 8):
            sbcopy(c, d).start()

    def ocopy(c):
        return pltpu.make_async_copy(ob.at[rs(c), :], out_ref.at[rs(c), :], osem)

    @named
    def f5(c, send):
        got(sb.at[c, pl.ds(0, 7)], sb_ss, sb_rs.at[c]).wait_recv()
        t = sb[c, 0]
        for i in range(1, 8):
            t = t + sb[c, i]
        if send:
            st[c] = t
            stcopy(c).start()
        ob[rs(c), :] = yg[rs(c), :] * scale_of(t, SIZES[c])
        ocopy(c).start()

    def when(c):
        return 0 <= c < count

    @pl.when(sec == 0)
    def _():
        ag1(g1, 0, 0)
        for k in range(4):
            slice_weights(k)
        ag2(g1, 0, 0)
        slice_weights(4)
        slice_weights(5)
        ag2b(g1, 0, 0)
        if when(1):
            ag1(g1, 0, 1)
        slice_weights(6)
        slice_weights(7)
        near_in(g1, 0, 0)
        prep(0, g1, NEAR)
        near(0, 2)
        ag3(g1, 0, 0)
        near(0, 1)
        far_in(g1, 0, 0)
        prep(0, g1, FAR)
        far(0, 2, False)
        far(0, 1, False)
        if when(1):
            ag2(g1, 0, 1)
        mm(0, 3)
        if when(1):
            ag2b(g1, 0, 1)
        if when(2):
            ag1(g1, 0, 2)
        mm(0, 0)
        if when(1):
            ag3(g1, 0, 1)
        f1(0)
        for c in range(1, count):
            near_in(g1, 0, c)
            far_in(g1, 0, c)
            prep(c, g1, ALL)
            mm(c, 2)
            if when(c + 1):
                ag2(g1, 0, c + 1)
                ag2b(g1, 0, c + 1)
            if when(c + 2):
                ag1(g1, 0, c + 2)
            if when(c - 2):
                f3(c - 2, True)
            mm(c, 1)
            if when(c - 3):
                f5(c - 3, True)
            mm(c, 3)
            f2(c - 1)
            mm(c, 0)
            if when(c + 1):
                ag3(g1, 0, c + 1)
            if when(c - 2):
                f4(c - 2)
            f1(c)
        n = count - 1
        f3(n - 1, True)
        f2(n)
        f5(n - 2, True)
        f4(n - 1)
        f3(n, True)
        f5(n - 1, True)
        f4(n)
        f5(n, True)
        got(yg, t_ss, t_rs.at[0]).wait_send()
        got(st, st_ss, st_rs.at[0]).wait_send()

    @pl.when(sec == 1)
    def _():
        wide = range(count, count + len(WIDE))
        ag1(g1, 0, wide[0])
        for k in range(4):
            slice_weights(k)
        ag2(g1, 0, wide[0])
        for k in range(4, 8):
            slice_weights(k)
        ag2b(g1, 0, wide[0])
        ag1(g1, 0, wide[1])
        ag3(g1, 0, wide[0])
        for c in wide:
            near_in(g1, 0, c)
            far_in(g1, 0, c)
            prep(c, g1, ALL)
            early(c, 2)
            if c + 1 in wide:
                ag2(g1, 0, c + 1)
            early(c, 1)
            if c + 1 in wide:
                ag2b(g1, 0, c + 1)
            if c + 2 in wide:
                ag1(g1, 0, c + 2)
            early(c, 3)
            if c + 1 in wide:
                ag3(g1, 0, c + 1)
            early(c, 0)

        @named
        def start(c):
            got(g2.at[r, rs(c), :], t_ss, t_rs.at[c]).wait_recv()
            ag1(g2, 1, c)

        start(0)
        ag2(g2, 1, 0)
        ag2b(g2, 1, 0)
        for c in range(count):
            if when(c + 1):
                start(c + 1)
            split = c in SPLIT
            if split:
                near_in(g2, 1, c)
                prep(c, g2, NEAR)
                near(c, 2)
                ag3(g2, 1, c)
                if when(c - 1):
                    f1(c - 1)
                near(c, 1)
            else:
                f1(c - 1)
                ag3(g2, 1, c)
                near_in(g2, 1, c)
            far_in(g2, 1, c)
            with jax.named_scope(f"stwait#a={c}"):
                got(sr.at[c], st_ss, st_rs.at[c]).wait_recv()
            scv[0 : SIZES[c], :] = scale_of(sr[c], SIZES[c])
            if split:
                prep(c, g2, FAR)
                far(c, 2, True)
            else:
                prep(c, g2, ALL)
                mm(c, 2, True)
            if when(c + 1):
                ag2(g2, 1, c + 1)
            if split:
                far(c, 1, True)
            else:
                mm(c, 1, True)
            if when(c + 1):
                ag2b(g2, 1, c + 1)
            mm(c, 3, True)
            if when(c - 1):
                f2(c - 1)
            mm(c, 0, True)
            if when(c - 2):
                f3(c - 2, False)
            if when(c - 3):
                f4(c - 3)
        n = count - 1
        f1(n)
        f3(n - 1, False)
        f4(n - 2)
        f2(n)
        for c in range(n - 2):
            f5(c, False)
        f4(n - 1)
        f3(n, False)
        f5(n - 2, False)
        f4(n)
        f5(n - 1, False)
        f5(n, False)
        got(g2.at[pl.ds(0, 7)], ag_s.at[1], ag_r.at[1, 0, 0]).wait_send()

    got(g1.at[pl.ds(0, 7)], ag_s.at[0], ag_r.at[0, 0, 0]).wait_send()
    got(p1s, p1_ss, p1_rs.at[0, 0]).wait_send()
    got(p2s, p2_ss, p2_rs.at[0]).wait_send()
    got(zs, z_ss, z_rs.at[0]).wait_send()
    got(sa.at[:, pl.ds(0, 7)], sa_ss, sa_rs.at[0]).wait_send()
    got(sb.at[:, pl.ds(0, 7)], sb_ss, sb_rs.at[0]).wait_send()
    pltpu.make_async_copy(ob, out_ref, osem).wait()


def shards(inputs, weights, norm_gain):
    micro, batch, piece = inputs.shape
    total = micro * batch
    width = weights.shape[-1]
    depth = weights.shape[1] * weights.shape[3]
    count = len(SIZES)
    rows = max(SIZES + WIDE)
    x = inputs.reshape(total, piece)
    w = weights.reshape(depth, width)
    blocks = width // piece
    dma = pltpu.SemaphoreType.DMA
    out = pl.pallas_call(
        kernel,
        out_shape=jax.ShapeDtypeStruct((total, piece), F32),
        in_specs=[
            pl.BlockSpec(memory_space=pl.ANY),
            pl.BlockSpec(memory_space=pl.ANY),
            pl.BlockSpec(memory_space=pltpu.VMEM),
        ],
        out_specs=pl.BlockSpec(memory_space=pl.ANY),
        scratch_shapes=[
            pltpu.VMEM((blocks, depth, piece), F32),
            pltpu.VMEM((blocks, depth, piece), BF16),
            pltpu.VMEM((blocks, depth, piece), BF16),
            pltpu.VMEM((2 * rows, depth), BF16),
            pltpu.VMEM((8, total, piece), F32),
            pltpu.VMEM((8, total, piece), F32),
            pltpu.VMEM((2, total, piece), F32),
            pltpu.VMEM((2, total, piece), F32),
            pltpu.VMEM((2, 2, total, piece), F32),
            pltpu.VMEM((2, 2, total, piece), F32),
            pltpu.VMEM((2, total, piece), F32),
            pltpu.VMEM((total, piece), F32),
            pltpu.VMEM((total, piece), F32),
            pltpu.VMEM((total, piece), F32),
            pltpu.VMEM((count, 8, 1, 128), F32),
            pltpu.VMEM((count, 8, 1, 128), F32),
            pltpu.VMEM((count, 1, 128), F32),
            pltpu.VMEM((count, 1, 128), F32),
            pltpu.VMEM((total, piece), F32),
            pltpu.VMEM((4, 2, total, piece), F32),
            pltpu.VMEM((rows, piece), F32),
            dma((8,)),
            dma(()),
            dma(()),
            dma((2,)),
            dma((2, count, 8)),
            dma(()),
            dma((count, 2)),
            dma(()),
            dma((count,)),
            dma(()),
            dma((count,)),
            dma(()),
            dma((count,)),
            dma(()),
            dma((count,)),
            dma(()),
            dma((count,)),
            dma(()),
            dma((count,)),
        ],
        compiler_params=pltpu.CompilerParams(
            collective_id=0, has_side_effects=True, vmem_limit_bytes=62 * 1024 * 1024
        ),
    )(x, w, norm_gain)
    return out.reshape(1, micro, batch, piece)


def solution(mesh):
    placed = (
        P(None, None, ("row", "col")),
        P("section", None, "col", None, "row"),
        P("section", ("row", "col")),
    )
    return jax.shard_map(
        shards,
        mesh=mesh,
        in_specs=placed,
        out_specs=P("section", None, None, ("row", "col")),
        check_vma=False,
    )
```
